8 devices in a mesh: dp: 2 (over z, y), sp: 4 (over x, core).
Axes of the slice: x: 2, y: 2, z: 1, core: 2. Of those that a mesh axis runs over, the one named last changes fastest.
Arguments:
- tokens: bfloat16 [16384, 384], P(('dp', 'sp')), parts along dimension 0
- grad_out: bfloat16 [16384, 384], P(('dp', 'sp')), parts along dimension 0
- ln_gain: float32 [384], replicated
- ln_bias: float32 [384], replicated
- w_qkv: bfloat16 [384, 1152], replicated
- w_out: bfloat16 [384, 384], replicated
- temperature: float32 [8], replicated
Outputs:
- output 1: bfloat16 [16384, 384], P(('dp', 'sp')), parts along dimension 0
- output 2: bfloat16 [16384, 384], P(('dp', 'sp')), parts along dimension 0
- output 3: float32 [768, 1152], P(('dp', 'sp')), parts along dimension 0
- output 4: float32 [768, 384], P(('dp', 'sp')), parts along dimension 0
- output 5: float32 [768], P('dp'), parts along dimension 0
- output 6: float32 [768], P('dp'), parts along dimension 0
- output 7: float32 [16], P('dp'), parts along dimension 0
There are 2 independent parts. The reference program is written for one: setup_inputs(seed, part) draws one part's arguments, and reference() takes and returns one part's arrays. A program takes and returns all parts, laid end to end along the dimension named above; an argument that names none is the same for every part.
All inputs are finite; a program needn't handle non-finite values.
Results may differ from the reference program's by a relative error of at most 0.00136218.
Values are sent between devices in bfloat16 or wider.
A program may use at most 1 GiB of HBM per device.

```python
import jax
import jax.numpy as jnp
from jax import lax

SEQ_LEN = 8192
MODEL_DIM = 384
NUM_HEADS = 8

HEAD_DIM = MODEL_DIM // NUM_HEADS


def setup_inputs(seed: int = 0, part: int = 0) -> dict:
    part_keys = jax.random.split(jax.random.fold_in(jax.random.key(seed), part), 4)
    shared_keys = jax.random.split(jax.random.key(seed + 1), 5)
    position = (jnp.arange(SEQ_LEN, dtype=jnp.float32) + 0.5) / SEQ_LEN
    wave_basis = jnp.cos(jnp.pi * position[:, None] * jnp.arange(1, 5, dtype=jnp.float32)[None, :])
    x_pattern = jnp.dot(wave_basis, jax.random.normal(part_keys[0], (4, MODEL_DIM), jnp.float32))
    tokens = jax.random.normal(part_keys[1], (SEQ_LEN, MODEL_DIM), jnp.float32) + x_pattern
    dy_pattern = jnp.dot(wave_basis, jax.random.normal(part_keys[2], (4, MODEL_DIM), jnp.float32))
    grad_out = jax.random.normal(part_keys[3], (SEQ_LEN, MODEL_DIM), jnp.float32) + 0.5 * dy_pattern
    w_scale = MODEL_DIM ** -0.5
    return {
        'tokens': tokens.astype(jnp.bfloat16),
        'grad_out': grad_out.astype(jnp.bfloat16),
        'ln_gain': 1.0 + 0.3 * jax.random.normal(shared_keys[0], (MODEL_DIM,), jnp.float32),
        'ln_bias': 0.3 * jax.random.normal(shared_keys[1], (MODEL_DIM,), jnp.float32),
        'w_qkv': (w_scale * jax.random.normal(shared_keys[2], (MODEL_DIM, 3 * MODEL_DIM), jnp.float32)).astype(jnp.bfloat16),
        'w_out': (w_scale * jax.random.normal(shared_keys[3], (MODEL_DIM, MODEL_DIM), jnp.float32)).astype(jnp.bfloat16),
        'temperature': jax.random.uniform(shared_keys[4], (NUM_HEADS,), jnp.float32, 2.5, 6.5),
    }


def layer_norm(x_f32, ln_gain, ln_bias):
    row_mean = jnp.mean(x_f32, axis=-1, keepdims=True)
    centered = x_f32 - row_mean
    row_var = jnp.mean(centered * centered, axis=-1, keepdims=True)
    return centered * lax.rsqrt(row_var + 1e-6) * ln_gain + ln_bias


def attn_probs(gram_sum, q_sq, k_sq, temperature):
    cosine = gram_sum / (jnp.sqrt(q_sq)[..., :, None] * jnp.sqrt(k_sq)[..., None, :])
    return jax.nn.softmax(temperature[..., None, None] * cosine, axis=-1)


def reference(tokens, grad_out, ln_gain, ln_bias, w_qkv, w_out, temperature):
    x_f32 = tokens.astype(jnp.float32)
    ln_value, ln_vjp = jax.vjp(layer_norm, x_f32, ln_gain, ln_bias)
    normed = ln_value.astype(jnp.bfloat16)
    qkv_act = jnp.dot(normed, w_qkv, preferred_element_type=jnp.float32).astype(jnp.bfloat16)
    qkv_heads = qkv_act.astype(jnp.float32).reshape(SEQ_LEN, 3, NUM_HEADS, HEAD_DIM)
    q_heads = qkv_heads[:, 0]
    k_heads = qkv_heads[:, 1]
    v_heads = qkv_heads[:, 2]
    gram_sum = jnp.einsum('nhi,nhj->hij', q_heads, k_heads)
    q_sq = jnp.sum(q_heads * q_heads, axis=0)
    k_sq = jnp.sum(k_heads * k_heads, axis=0)
    attn_f32, probs_vjp = jax.vjp(attn_probs, gram_sum, q_sq, k_sq, temperature)
    attn_weights = attn_f32.astype(jnp.bfloat16).astype(jnp.float32)
    attn_out = jnp.einsum('nhj,hij->nhi', v_heads, attn_weights).astype(jnp.bfloat16).reshape(SEQ_LEN, MODEL_DIM)
    out_tokens = (x_f32 + jnp.dot(attn_out, w_out, preferred_element_type=jnp.float32)).astype(jnp.bfloat16)

    grad_w_out = jnp.dot(attn_out.T, grad_out, preferred_element_type=jnp.float32)
    d_attn = jnp.dot(grad_out, w_out.T, preferred_element_type=jnp.float32).astype(jnp.bfloat16)
    d_heads = d_attn.astype(jnp.float32).reshape(SEQ_LEN, NUM_HEADS, HEAD_DIM)
    d_probs = jnp.einsum('nhi,nhj->hij', d_heads, v_heads)
    d_gram, d_qsq, d_ksq, grad_temperature = probs_vjp(d_probs)
    d_gram_bf = d_gram.astype(jnp.bfloat16).astype(jnp.float32)
    d_q = jnp.einsum('hij,nhj->nhi', d_gram_bf, k_heads) + 2.0 * q_heads * d_qsq
    d_k = jnp.einsum('hij,nhi->nhj', d_gram_bf, q_heads) + 2.0 * k_heads * d_ksq
    d_v = jnp.einsum('hij,nhi->nhj', attn_weights, d_heads)
    d_qkv = jnp.stack([d_q, d_k, d_v], axis=1).astype(jnp.bfloat16).reshape(SEQ_LEN, 3 * MODEL_DIM)
    grad_w_qkv = jnp.dot(normed.T, d_qkv, preferred_element_type=jnp.float32)
    d_normed = jnp.dot(d_qkv, w_qkv.T, preferred_element_type=jnp.float32)
    d_x, grad_gain, grad_bias = ln_vjp(d_normed)
    grad_tokens = (grad_out.astype(jnp.float32) + d_x).astype(jnp.bfloat16)
    return (out_tokens, grad_tokens, grad_w_qkv, grad_w_out, grad_gain, grad_bias, grad_temperature)
```

```python
import functools

import jax
import jax.numpy as jnp
from jax import lax
from jax.experimental import pallas as pl
from jax.experimental.pallas import tpu as pltpu
from jax.sharding import PartitionSpec as P

F32, BF16 = jnp.float32, jnp.bfloat16
MESH = pl.DeviceIdType.MESH
BM = 512


def dot_nn(a, b):
    return lax.dot_general(a, b, (((1,), (0,)), ((), ())), preferred_element_type=F32)


def dot_nt(a, b):
    return lax.dot_general(a, b, (((1,), (1,)), ((), ())), preferred_element_type=F32)


def dot_tn(a, b):
    return lax.dot_general(a, b, (((0,), (0,)), ((), ())), preferred_element_type=F32)


def kernel(num_heads, num_sp,
           x_hbm, dy_hbm, gain_ref, bias_ref, wqkv_hbm, wout_hbm, temp_ref,
           out_hbm, gtok_hbm, gwqkv_ref, gwout_ref, ggain_ref, gbias_ref, gtemp_ref,
           x_v, dy_v, wqkv, wout, u_v, ut_v, xhat, rstd, q_v, k_v, v_v, do_v, o_v, dqkv, out_st, gt_st,
           acc, abd, gbd, g_own, g_rx1, g_sum, g_rx2, d_own, d_rx1, d_sum, d_rx2,
           gw, w_rx1, w_sum, w_rx2, gb,
           in_sem, out_sem, gs, gr, ws, wr, bs, br):
    rows_n, dim = x_v.shape
    hd = dim // num_heads
    nb = rows_n // BM
    wrows = dim // num_sp

    me = lax.axis_index('sp')
    partner = me + 1 - 2 * lax.rem(me, 2)
    peer = lax.rem(me + 2, 4)
    diag = lax.rem(partner + 2, 4)

    barrier = pltpu.get_barrier_semaphore()
    for other in (partner, peer, diag):
        pl.semaphore_signal(barrier, inc=1, device_id={'sp': other}, device_id_type=MESH)

    def block(i):
        return pl.ds(pl.multiple_of(i * BM, BM), BM)

    def x_copy(i):
        return pltpu.make_async_copy(x_hbm.at[block(i)], x_v.at[block(i)], in_sem.at[i])

    def dy_copy(i):
        return pltpu.make_async_copy(dy_hbm.at[block(i)], dy_v.at[block(i)], in_sem.at[nb + i])

    wq_copy = pltpu.make_async_copy(wqkv_hbm, wqkv, in_sem.at[2 * nb])
    wo_copy = pltpu.make_async_copy(wout_hbm, wout, in_sem.at[2 * nb + 1])
    x_copy(0).start()
    wq_copy.start()
    for i in range(1, nb):
        x_copy(i).start()
    wo_copy.start()
    for i in range(nb):
        dy_copy(i).start()

    lane = lax.broadcasted_iota(jnp.int32, (hd, dim), 1)
    row = lax.broadcasted_iota(jnp.int32, (hd, dim), 0)
    head_mask = [(lane >= h * hd) & (lane < (h + 1) * hd) for h in range(num_heads)]

    def fold(full_ref):
        total = jnp.zeros((hd, dim), F32)
        for h in range(num_heads):
            total = jnp.where(head_mask[h], full_ref[h * hd:(h + 1) * hd, :], total)
        return total

    def expand(ref, compact):
        for h in range(num_heads):
            ref[h * hd:(h + 1) * hd, :] = jnp.where(head_mask[h], compact, 0.0).astype(BF16)

    def send(src, dst, ssem, rsem, dev):
        return pltpu.make_async_remote_copy(src_ref=src, dst_ref=dst, send_sem=ssem, recv_sem=rsem,
                                            device_id={'sp': dev}, device_id_type=MESH)

    gain = gain_ref[...].reshape(1, dim)
    bias = bias_ref[...].reshape(1, dim)
    inv_d = 1.0 / dim

    wq_copy.wait()

    acc[...] = jnp.zeros_like(acc)

    def p1(i, carry):
        sq, sk = carry
        r = block(i)
        x_copy(i).wait()
        xf = x_v[r, :].astype(F32)
        cen = xf - jnp.sum(xf, axis=-1, keepdims=True) * inv_d
        var = jnp.sum(cen * cen, axis=-1, keepdims=True) * inv_d
        rs = lax.rsqrt(var + 1e-6)
        xh = cen * rs
        xhat[r, :] = xh
        rstd[r, :] = jnp.broadcast_to(rs, (BM, 128))
        u = (xh * gain + bias).astype(BF16)
        u_v[r, :] = u
        qk = dot_nn(u, wqkv[:, :2 * dim]).astype(BF16)
        q, k = qk[:, :dim], qk[:, dim:]
        q_v[r, :] = q
        k_v[r, :] = k
        acc[...] += dot_tn(k, q)
        qf, kf = q.astype(F32), k.astype(F32)
        sq = sq + jnp.sum((qf * qf).reshape(BM // 8, 8, dim), axis=0)
        sk = sk + jnp.sum((kf * kf).reshape(BM // 8, 8, dim), axis=0)
        return sq, sk

    zero8 = jnp.zeros((8, dim), F32)
    sq, sk = lax.fori_loop(0, nb, p1, (zero8, zero8))
    g_own[:hd, :] = fold(acc)
    row8 = lax.broadcasted_iota(jnp.int32, (8, dim), 0)
    g_own[hd:hd + 8, :] = jnp.where(row8 == 0, jnp.sum(sq, axis=0, keepdims=True),
                                    jnp.where(row8 == 1, jnp.sum(sk, axis=0, keepdims=True), 0.0))

    pl.semaphore_wait(barrier, 3)
    g1 = send(g_own, g_rx1, gs.at[0], gr.at[0], partner)
    g1.start()

    acc[...] = jnp.zeros_like(acc)
    wo_copy.wait()

    def p2(i, carry):
        r = block(i)
        dy_copy(i).wait()
        u = u_v[r, :]
        v = dot_nn(u, wqkv[:, 2 * dim:]).astype(BF16)
        v_v[r, :] = v
        do = dot_nt(dy_v[r, :], wout[...]).astype(BF16)
        do_v[r, :] = do
        acc[...] += dot_tn(v, do)
        ut_v[:, r] = u.T
        return carry

    lax.fori_loop(0, nb // 2, p2, 0)
    g1.wait()
    g_sum[...] = g_own[...] + g_rx1[...]
    g2 = send(g_sum, g_rx2, gs.at[1], gr.at[1], peer)
    g2.start()
    lax.fori_loop(nb // 2, nb, p2, 0)

    d_own[...] = fold(acc)
    d1 = send(d_own, d_rx1, gs.at[2], gr.at[2], partner)
    d1.start()
    d1.wait()
    d_sum[...] = d_own[...] + d_rx1[...]
    d2 = send(d_sum, d_rx2, gs.at[3], gr.at[3], peer)
    d2.start()

    g2.wait()
    tot = g_sum[...] + g_rx2[...]
    gram = tot[:hd, :]
    sq_row = tot[hd:hd + 1, :]
    sk_row = tot[hd + 1:hd + 2, :]
    sk_full = jnp.zeros((hd, dim), F32)
    for h in range(num_heads):
        col = jnp.sum(jnp.where(lane == row + h * hd, sk_row, 0.0), axis=1, keepdims=True)
        sk_full = jnp.where(head_mask[h], col, sk_full)
    tau = jnp.zeros((1, dim), F32)
    for h in range(num_heads):
        tau = jnp.where(head_mask[h][:1, :], temp_ref[h], tau)
    denom = jnp.sqrt(sq_row) * jnp.sqrt(sk_full)
    cos = gram / denom
    s = tau * cos
    e = jnp.exp(s - jnp.max(s, axis=0, keepdims=True))
    prob = e / jnp.sum(e, axis=0, keepdims=True)
    expand(abd, prob)

    def pair_send(c, part):
        rows = pl.ds(pl.multiple_of((partner if part else diag) * wrows, 8), wrows)
        return send(gw.at[c, rows, :], w_rx1.at[c, part], ws.at[3 * c + part], wr.at[3 * c + part], partner)

    def cross_send(c):
        return send(w_sum.at[c], w_rx2.at[c], ws.at[3 * c + 2], wr.at[3 * c + 2], peer)

    def pair_start(c):
        pair_send(c, 0).start()
        pair_send(c, 1).start()

    def cross_start(c):
        pair_send(c, 0).wait()
        w_sum[c] = gw[c, pl.ds(pl.multiple_of(peer * wrows, 8), wrows), :] + w_rx1[c, 0]
        cross_send(c).start()

    def p3(i, carry):
        r = block(i)
        dqkv[r, 2 * dim:] = dot_nt(do_v[r, :], abd[...]).astype(BF16)
        return carry

    lax.fori_loop(0, nb, p3, 0)
    gw[2] = dot_nn(ut_v[...], dqkv[:, 2 * dim:])
    pair_start(2)

    def p4(i, carry):
        r = block(i)
        o_v[r, :] = dot_nn(v_v[r, :], abd[...]).astype(BF16)
        return carry

    lax.fori_loop(0, nb, p4, 0)
    cross_start(2)
    gw[3] = dot_tn(o_v[...], dy_v[...])
    pair_start(3)

    d2.wait()
    da = d_sum[...] + d_rx2[...]
    ds = prob * (da - jnp.sum(prob * da, axis=0, keepdims=True))
    dcos = tau * ds
    t_row = jnp.sum(ds * cos, axis=0, keepdims=True)
    lane_t = lax.broadcasted_iota(jnp.int32, (1, num_heads), 1)
    g_temp = jnp.zeros((1, num_heads), F32)
    for h in range(num_heads):
        val = jnp.sum(jnp.where(head_mask[h][:1, :], t_row, 0.0), axis=1, keepdims=True)
        g_temp = jnp.where(lane_t == h, val, g_temp)
    gtemp_ref[...] = g_temp
    expand(gbd, dcos / denom)
    z = dcos * cos
    dsq2 = -jnp.sum(z, axis=0, keepdims=True) / sq_row
    sk_grad = jnp.zeros((hd, dim), F32)
    for h in range(num_heads):
        col = jnp.sum(jnp.where(head_mask[h], z, 0.0), axis=1, keepdims=True)
        sk_grad = jnp.where(lane == row + h * hd, col, sk_grad)
    dsk2 = -jnp.sum(sk_grad, axis=0, keepdims=True) / sk_row

    def p5(i, carry):
        r = block(i)
        dqkv[r, :dim] = (dot_nn(k_v[r, :], gbd[...]) + q_v[r, :].astype(F32) * dsq2).astype(BF16)
        return carry

    lax.fori_loop(0, nb, p5, 0)
    cross_start(3)
    gw[0] = dot_nn(ut_v[...], dqkv[:, :dim])
    pair_start(0)

    def p6(i, carry):
        r = block(i)
        dqkv[r, dim:2 * dim] = (dot_nt(q_v[r, :], gbd[...]) + k_v[r, :].astype(F32) * dsk2).astype(BF16)
        return carry

    lax.fori_loop(0, nb, p6, 0)
    cross_start(0)
    gw[1] = dot_nn(ut_v[...], dqkv[:, dim:2 * dim])
    pair_start(1)

    def out_copy(i):
        return pltpu.make_async_copy(out_st.at[block(i)], out_hbm.at[block(i)], out_sem.at[i])

    def gt_copy(i):
        return pltpu.make_async_copy(gt_st.at[block(i)], gtok_hbm.at[block(i)], out_sem.at[nb + i])

    def p7(i, carry):
        r = block(i)
        y = dot_nn(o_v[r, :], wout[...])
        out_st[r, :] = (x_v[r, :].astype(F32) + y).astype(BF16)
        out_copy(i).start()
        return carry

    lax.fori_loop(0, nb, p7, 0)
    cross_start(1)

    def p8(i, carry):
        gg, gbi = carry
        r = block(i)
        du = dot_nt(dqkv[r, :], wqkv[...])
        xh = xhat[r, :]
        dux = du * xh
        gg = gg + jnp.sum(dux.reshape(BM // 8, 8, dim), axis=0)
        gbi = gbi + jnp.sum(du.reshape(BM // 8, 8, dim), axis=0)
        m1 = jnp.sum(du * gain, axis=-1, keepdims=True) * inv_d
        m2 = jnp.sum(dux * gain, axis=-1, keepdims=True) * inv_d
        dx = (du * gain - m1 - xh * m2) * rstd[r, :1]
        gt_st[r, :] = (dy_v[r, :].astype(F32) + dx).astype(BF16)
        gt_copy(i).start()
        return gg, gbi

    gg, gbi = lax.fori_loop(0, nb, p8, (zero8, zero8))
    gb[me] = jnp.where(row8 == 0, jnp.sum(gg, axis=0, keepdims=True),
                       jnp.where(row8 == 1, jnp.sum(gbi, axis=0, keepdims=True), 0.0))
    gbc = [send(gb.at[me], gb.at[me], bs.at[n], br.at[n], other) for n, other in enumerate((partner, peer, diag))]
    for c in gbc:
        c.start()

    mine = pl.ds(pl.multiple_of(me * wrows, 8), wrows)
    for c in (2, 3, 0, 1):
        pair_send(c, 1).wait()
        cross_send(c).wait()
        total = gw[c, mine, :] + w_rx1[c, 1] + w_rx2[c]
        if c == 3:
            gwout_ref[...] = total
        else:
            gwqkv_ref[:, c * dim:(c + 1) * dim] = total
    for c in gbc:
        c.wait()
    gsum = (gb[0] + gb[1]) + (gb[2] + gb[3])
    ggain_ref[...] = gsum[0:1, :]
    gbias_ref[...] = gsum[1:2, :]

    def drain(i, carry):
        out_copy(i).wait()
        gt_copy(i).wait()
        return carry

    lax.fori_loop(0, nb, drain, 0)


def solution(mesh):
    row_spec = P(('dp', 'sp'), None)
    part_spec = P('dp')
    full_spec = P()
    num_sp = mesh.shape['sp']

    def local_step(x, dy, gain, bias, w_qkv, w_out, temperature):
        n, d = x.shape
        h = temperature.shape[0]
        hd = d // h
        wrows = d // num_sp
        nb = n // BM
        vmem = pl.BlockSpec(memory_space=pltpu.VMEM)
        smem = pl.BlockSpec(memory_space=pltpu.SMEM)
        hbm = pl.BlockSpec(memory_space=pl.ANY)
        tok = pltpu.VMEM((n, d), BF16)
        sds = jax.ShapeDtypeStruct
        dma = pltpu.SemaphoreType.DMA
        outs = pl.pallas_call(
            functools.partial(kernel, h, num_sp),
            name='xca',
            out_shape=(sds((n, d), BF16), sds((n, d), BF16), sds((wrows, 3 * d), F32), sds((wrows, d), F32),
                       sds((1, d), F32), sds((1, d), F32), sds((1, h), F32)),
            in_specs=[hbm, hbm, vmem, vmem, hbm, hbm, smem],
            out_specs=(hbm, hbm, vmem, vmem, vmem, vmem, vmem),
            scratch_shapes=[
                tok, tok, pltpu.VMEM((d, 3 * d), BF16), pltpu.VMEM((d, d), BF16), tok, pltpu.VMEM((d, n), BF16),
                pltpu.VMEM((n, d), F32), pltpu.VMEM((n, 128), F32), tok, tok, tok, tok, tok,
                pltpu.VMEM((n, 3 * d), BF16), tok, tok,
                pltpu.VMEM((d, d), F32), pltpu.VMEM((d, d), BF16), pltpu.VMEM((d, d), BF16),
                pltpu.VMEM((hd + 8, d), F32), pltpu.VMEM((hd + 8, d), F32), pltpu.VMEM((hd + 8, d), F32),
                pltpu.VMEM((hd + 8, d), F32),
                pltpu.VMEM((hd, d), F32), pltpu.VMEM((hd, d), F32), pltpu.VMEM((hd, d), F32), pltpu.VMEM((hd, d), F32),
                pltpu.VMEM((4, d, d), F32), pltpu.VMEM((4, 2, wrows, d), F32), pltpu.VMEM((4, wrows, d), F32),
                pltpu.VMEM((4, wrows, d), F32), pltpu.VMEM((4, 8, d), F32),
                dma((2 * nb + 2,)), dma((2 * nb,)), dma((4,)), dma((4,)), dma((12,)), dma((12,)), dma((3,)), dma((3,)),
            ],
            compiler_params=pltpu.CompilerParams(collective_id=0, has_side_effects=True,
                                                 vmem_limit_bytes=60 * 1024 * 1024),
        )(x, dy, gain, bias, w_qkv, w_out, temperature)
        out, gtok, gwqkv, gwout, ggain, gbias, gtemp = outs
        return out, gtok, gwqkv, gwout, ggain.reshape(d), gbias.reshape(d), gtemp.reshape(h)

    return jax.shard_map(local_step, mesh=mesh,
                         in_specs=(row_spec, row_spec, full_spec, full_spec, full_spec, full_spec, full_spec),
                         out_specs=(row_spec, row_spec, row_spec, row_spec, part_spec, part_spec, part_spec),
                         check_vma=False)
```

```python
import functools

import jax
import jax.numpy as jnp
from jax import lax
from jax.experimental import pallas as pl
from jax.experimental.pallas import tpu as pltpu
from jax.sharding import PartitionSpec as P

F32, BF16 = jnp.float32, jnp.bfloat16
MESH = pl.DeviceIdType.MESH
BM = 512


def dot_nn(a, b):
    return lax.dot_general(a, b, (((1,), (0,)), ((), ())), preferred_element_type=F32)


def dot_nt(a, b):
    return lax.dot_general(a, b, (((1,), (1,)), ((), ())), preferred_element_type=F32)


def dot_tn(a, b):
    return lax.dot_general(a, b, (((0,), (0,)), ((), ())), preferred_element_type=F32)


def kernel(num_heads, num_sp,
           x_hbm, dy_hbm, gain_hbm, bias_hbm, wqkv_hbm, wout_hbm, temp_hbm,
           out_st, gt_st, gwqkv_ref, gwout_ref, ggain_ref, gbias_ref, gtemp_ref,
           gain_ref, bias_ref, temp_ref, x_v, dy_v, wqkv, wout, u_v, ut_v, xhat, rstd, q_v, k_v, v_v, do_v, o_v, dqkv,
           acc, abd, gbd, g_own, g_rx1, g_sum, g_rx2, d_own, d_rx1, d_sum, d_rx2,
           gw, w_rx1, w_sum, w_rx2, gb,
           in_sem, gs, gr, ws, wr, bs, br):
    rows_n, dim = x_v.shape
    hd = dim // num_heads
    nb = rows_n // BM
    wrows = dim // num_sp

    me = lax.axis_index('sp')
    partner = me + 1 - 2 * lax.rem(me, 2)
    peer = lax.rem(me + 2, 4)
    diag = lax.rem(partner + 2, 4)

    barrier = pltpu.get_barrier_semaphore()
    for other in (partner, peer, diag):
        pl.semaphore_signal(barrier, inc=1, device_id={'sp': other}, device_id_type=MESH)

    def block(i):
        return pl.ds(pl.multiple_of(i * BM, BM), BM)

    def x_copy(i):
        return pltpu.make_async_copy(x_hbm.at[block(i)], x_v.at[block(i)], in_sem.at[i])

    def dy_copy(i):
        return pltpu.make_async_copy(dy_hbm.at[block(i)], dy_v.at[block(i)], in_sem.at[nb + i])

    wq_copy = pltpu.make_async_copy(wqkv_hbm, wqkv, in_sem.at[2 * nb])
    wo_copy = pltpu.make_async_copy(wout_hbm, wout, in_sem.at[2 * nb + 1])
    small = [pltpu.make_async_copy(a, b, in_sem.at[2 * nb + 2 + n]) for n, (a, b) in enumerate(
        ((gain_hbm, gain_ref), (bias_hbm, bias_ref), (temp_hbm, temp_ref)))]
    x_copy(0).start()
    for c in small:
        c.start()
    wq_copy.start()
    for i in range(1, nb):
        x_copy(i).start()
    wo_copy.start()
    for i in range(nb):
        dy_copy(i).start()

    lane = lax.broadcasted_iota(jnp.int32, (hd, dim), 1)
    row = lax.broadcasted_iota(jnp.int32, (hd, dim), 0)
    head_mask = [(lane >= h * hd) & (lane < (h + 1) * hd) for h in range(num_heads)]

    def fold(full_ref):
        total = jnp.zeros((hd, dim), F32)
        for h in range(num_heads):
            total = jnp.where(head_mask[h], full_ref[h * hd:(h + 1) * hd, :], total)
        return total

    def expand(ref, compact):
        for h in range(num_heads):
            ref[h * hd:(h + 1) * hd, :] = jnp.where(head_mask[h], compact, 0.0).astype(BF16)

    def send(src, dst, ssem, rsem, dev):
        return pltpu.make_async_remote_copy(src_ref=src, dst_ref=dst, send_sem=ssem, recv_sem=rsem,
                                            device_id={'sp': dev}, device_id_type=MESH)

    for c in small:
        c.wait()
    gain = gain_ref[...].reshape(1, dim)
    bias = bias_ref[...].reshape(1, dim)
    inv_d = 1.0 / dim

    wq_copy.wait()

    acc[...] = jnp.zeros_like(acc)

    def p1(i, carry):
        sq, sk = carry
        r = block(i)
        x_copy(i).wait()
        xf = x_v[r, :].astype(F32)
        cen = xf - jnp.sum(xf, axis=-1, keepdims=True) * inv_d
        var = jnp.sum(cen * cen, axis=-1, keepdims=True) * inv_d
        rs = lax.rsqrt(var + 1e-6)
        xh = cen * rs
        xhat[r, :] = xh
        rstd[r, :] = jnp.broadcast_to(rs, (BM, 128))
        u = (xh * gain + bias).astype(BF16)
        u_v[r, :] = u
        qk = dot_nn(u, wqkv[:, :2 * dim]).astype(BF16)
        q, k = qk[:, :dim], qk[:, dim:]
        q_v[r, :] = q
        k_v[r, :] = k
        acc[...] += dot_tn(k, q)
        qf, kf = q.astype(F32), k.astype(F32)
        sq = sq + jnp.sum((qf * qf).reshape(BM // 8, 8, dim), axis=0)
        sk = sk + jnp.sum((kf * kf).reshape(BM // 8, 8, dim), axis=0)
        return sq, sk

    zero8 = jnp.zeros((8, dim), F32)
    with jax.named_scope('p1'):
        sq, sk = lax.fori_loop(0, nb, p1, (zero8, zero8))
    g_own[:hd, :] = fold(acc)
    row8 = lax.broadcasted_iota(jnp.int32, (8, dim), 0)
    g_own[hd:hd + 8, :] = jnp.where(row8 == 0, jnp.sum(sq, axis=0, keepdims=True),
                                    jnp.where(row8 == 1, jnp.sum(sk, axis=0, keepdims=True), 0.0))

    with jax.named_scope('barw'):
        pl.semaphore_wait(barrier, 3)
    g1 = send(g_own, g_rx1, gs.at[0], gr.at[0], partner)
    g1.start()

    acc[...] = jnp.zeros_like(acc)
    wo_copy.wait()

    def p2(i, carry):
        r = block(i)
        dy_copy(i).wait()
        u = u_v[r, :]
        v = dot_nn(u, wqkv[:, 2 * dim:]).astype(BF16)
        v_v[r, :] = v
        do = dot_nt(dy_v[r, :], wout[...]).astype(BF16)
        do_v[r, :] = do
        acc[...] += dot_tn(v, do)
        ut_v[:, r] = u.T
        return carry

    with jax.named_scope('p2a'):
        lax.fori_loop(0, nb // 2, p2, 0)
    with jax.named_scope('g1w'):
        g1.wait()
    g_sum[...] = g_own[...] + g_rx1[...]
    g2 = send(g_sum, g_rx2, gs.at[1], gr.at[1], peer)
    g2.start()
    with jax.named_scope('p2b'):
        lax.fori_loop(nb // 2, nb, p2, 0)

    d_own[...] = fold(acc)
    d1 = send(d_own, d_rx1, gs.at[2], gr.at[2], partner)
    d1.start()
    with jax.named_scope('d1w'):
        d1.wait()
    d_sum[...] = d_own[...] + d_rx1[...]
    d2 = send(d_sum, d_rx2, gs.at[3], gr.at[3], peer)
    d2.start()

    with jax.named_scope('g2w'):
        g2.wait()
    tot = g_sum[...] + g_rx2[...]
    gram = tot[:hd, :]
    sq_row = tot[hd:hd + 1, :]
    sk_row = tot[hd + 1:hd + 2, :]
    sk_full = jnp.zeros((hd, dim), F32)
    for h in range(num_heads):
        col = jnp.sum(jnp.where(lane == row + h * hd, sk_row, 0.0), axis=1, keepdims=True)
        sk_full = jnp.where(head_mask[h], col, sk_full)
    tau = jnp.zeros((1, dim), F32)
    for h in range(num_heads):
        tau = jnp.where(head_mask[h][:1, :], temp_ref[h], tau)
    denom = jnp.sqrt(sq_row) * jnp.sqrt(sk_full)
    cos = gram / denom
    s = tau * cos
    e = jnp.exp(s - jnp.max(s, axis=0, keepdims=True))
    prob = e / jnp.sum(e, axis=0, keepdims=True)
    expand(abd, prob)

    def pair_send(c, part):
        rows = pl.ds(pl.multiple_of((partner if part else diag) * wrows, 8), wrows)
        return send(gw.at[c, rows, :], w_rx1.at[c, part], ws.at[3 * c + part], wr.at[3 * c + part], partner)

    def cross_send(c):
        return send(w_sum.at[c], w_rx2.at[c], ws.at[3 * c + 2], wr.at[3 * c + 2], peer)

    def pair_start(c):
        pair_send(c, 0).start()
        pair_send(c, 1).start()

    def cross_start(c):
        pair_send(c, 0).wait()
        w_sum[c] = gw[c, pl.ds(pl.multiple_of(peer * wrows, 8), wrows), :] + w_rx1[c, 0]
        cross_send(c).start()

    def p3(i, carry):
        r = block(i)
        dqkv[r, 2 * dim:] = dot_nt(do_v[r, :], abd[...]).astype(BF16)
        return carry

    with jax.named_scope('p3'):
        lax.fori_loop(0, nb, p3, 0)
    with jax.named_scope('gw2'):
        gw[2] = dot_nn(ut_v[...], dqkv[:, 2 * dim:])
    pair_start(2)

    def p4(i, carry):
        r = block(i)
        o_v[r, :] = dot_nn(v_v[r, :], abd[...]).astype(BF16)
        return carry

    with jax.named_scope('p4'):
        lax.fori_loop(0, nb, p4, 0)
    with jax.named_scope('cs2'):
        cross_start(2)
    with jax.named_scope('gw3'):
        gw[3] = dot_tn(o_v[...], dy_v[...])
    pair_start(3)

    with jax.named_scope('d2w'):
        d2.wait()
    da = d_sum[...] + d_rx2[...]
    ds = prob * (da - jnp.sum(prob * da, axis=0, keepdims=True))
    dcos = tau * ds
    t_row = jnp.sum(ds * cos, axis=0, keepdims=True)
    lane_t = lax.broadcasted_iota(jnp.int32, (1, num_heads), 1)
    g_temp = jnp.zeros((1, num_heads), F32)
    for h in range(num_heads):
        val = jnp.sum(jnp.where(head_mask[h][:1, :], t_row, 0.0), axis=1, keepdims=True)
        g_temp = jnp.where(lane_t == h, val, g_temp)
    gtemp_ref[...] = g_temp
    expand(gbd, dcos / denom)
    z = dcos * cos
    dsq2 = -jnp.sum(z, axis=0, keepdims=True) / sq_row
    sk_grad = jnp.zeros((hd, dim), F32)
    for h in range(num_heads):
        col = jnp.sum(jnp.where(head_mask[h], z, 0.0), axis=1, keepdims=True)
        sk_grad = jnp.where(lane == row + h * hd, col, sk_grad)
    dsk2 = -jnp.sum(sk_grad, axis=0, keepdims=True) / sk_row

    def p5(i, carry):
        r = block(i)
        dqkv[r, :dim] = (dot_nn(k_v[r, :], gbd[...]) + q_v[r, :].astype(F32) * dsq2).astype(BF16)
        return carry

    with jax.named_scope('p5'):
        lax.fori_loop(0, nb, p5, 0)
    with jax.named_scope('cs3'):
        cross_start(3)
    with jax.named_scope('gw0'):
        gw[0] = dot_nn(ut_v[...], dqkv[:, :dim])
    pair_start(0)

    def p6(i, carry):
        r = block(i)
        dqkv[r, dim:2 * dim] = (dot_nt(q_v[r, :], gbd[...]) + k_v[r, :].astype(F32) * dsk2).astype(BF16)
        return carry

    with jax.named_scope('p6'):
        lax.fori_loop(0, nb, p6, 0)
    with jax.named_scope('cs0'):
        cross_start(0)
    with jax.named_scope('gw1'):
        gw[1] = dot_nn(ut_v[...], dqkv[:, dim:2 * dim])
    pair_start(1)

    def p7(i, carry):
        r = block(i)
        y = dot_nn(o_v[r, :], wout[...])
        out_st[r, :] = (x_v[r, :].astype(F32) + y).astype(BF16)
        return carry

    with jax.named_scope('p7'):
        lax.fori_loop(0, nb, p7, 0)
    with jax.named_scope('cs1'):
        cross_start(1)

    def p8(i, carry):
        gg, gbi = carry
        r = block(i)
        du = dot_nt(dqkv[r, :], wqkv[...])
        xh = xhat[r, :]
        dux = du * xh
        gg = gg + jnp.sum(dux.reshape(BM // 8, 8, dim), axis=0)
        gbi = gbi + jnp.sum(du.reshape(BM // 8, 8, dim), axis=0)
        m1 = jnp.sum(du * gain, axis=-1, keepdims=True) * inv_d
        m2 = jnp.sum(dux * gain, axis=-1, keepdims=True) * inv_d
        dx = (du * gain - m1 - xh * m2) * rstd[r, :1]
        gt_st[r, :] = (dy_v[r, :].astype(F32) + dx).astype(BF16)
        return gg, gbi

    with jax.named_scope('p8'):
        gg, gbi = lax.fori_loop(0, nb, p8, (zero8, zero8))
    gb[me] = jnp.where(row8 == 0, jnp.sum(gg, axis=0, keepdims=True),
                       jnp.where(row8 == 1, jnp.sum(gbi, axis=0, keepdims=True), 0.0))
    gbc = [send(gb.at[me], gb.at[me], bs.at[n], br.at[n], other) for n, other in enumerate((partner, peer, diag))]
    for c in gbc:
        c.start()

    mine = pl.ds(pl.multiple_of(me * wrows, 8), wrows)
    for c in (2, 3, 0, 1):
        with jax.named_scope(f'fin{c}'):
            pair_send(c, 1).wait()
            cross_send(c).wait()
        total = gw[c, mine, :] + w_rx1[c, 1] + w_rx2[c]
        if c == 3:
            gwout_ref[...] = total
        else:
            gwqkv_ref[:, c * dim:(c + 1) * dim] = total
    with jax.named_scope('gbw'):
        for c in gbc:
            c.wait()
    gsum = (gb[0] + gb[1]) + (gb[2] + gb[3])
    ggain_ref[...] = gsum[0:1, :]
    gbias_ref[...] = gsum[1:2, :]


def finish(out_v, gt_v, gwqkv_v, gwout_v, ggain_v, gbias_v, gtemp_v,
           out_hbm, gt_hbm, gwqkv_hbm, gwout_hbm, ggain_ref, gbias_ref, gtemp_ref, sem):
    pairs = ((out_v, out_hbm), (gt_v, gt_hbm), (gwqkv_v, gwqkv_hbm), (gwout_v, gwout_hbm))
    copies = [pltpu.make_async_copy(src, dst, sem.at[n]) for n, (src, dst) in enumerate(pairs)]
    for c in copies:
        c.start()
    for src, dst in ((ggain_v, ggain_ref), (gbias_v, gbias_ref), (gtemp_v, gtemp_ref)):
        dst[...] = src[...].reshape(dst.shape)
    for c in copies:
        c.wait()


def solution(mesh):
    row_spec = P(('dp', 'sp'), None)
    part_spec = P('dp')
    full_spec = P()
    num_sp = mesh.shape['sp']

    def local_step(x, dy, gain, bias, w_qkv, w_out, temperature):
        n, d = x.shape
        h = temperature.shape[0]
        hd = d // h
        wrows = d // num_sp
        nb = n // BM
        vmem = pl.BlockSpec(memory_space=pltpu.VMEM)
        hbm = pl.BlockSpec(memory_space=pltpu.HBM)
        tok = pltpu.VMEM((n, d), BF16)
        sds = jax.ShapeDtypeStruct
        dma = pltpu.SemaphoreType.DMA
        in_hbm = functools.partial(pltpu.with_memory_space_constraint, memory_space=pltpu.HBM)
        outs = pl.pallas_call(
            functools.partial(kernel, h, num_sp),
            name='xca',
            out_shape=(pltpu.VMEM((n, d), BF16), pltpu.VMEM((n, d), BF16), pltpu.VMEM((wrows, 3 * d), F32),
                       pltpu.VMEM((wrows, d), F32), pltpu.VMEM((1, d), F32), pltpu.VMEM((1, d), F32),
                       pltpu.VMEM((1, h), F32)),
            in_specs=[hbm] * 7,
            out_specs=(vmem,) * 7,
            scratch_shapes=[
                pltpu.VMEM((d,), F32), pltpu.VMEM((d,), F32), pltpu.SMEM((h,), F32), tok, tok, pltpu.VMEM((d, 3 * d), BF16), pltpu.VMEM((d, d), BF16), tok, pltpu.VMEM((d, n), BF16),
                pltpu.VMEM((n, d), F32), pltpu.VMEM((n, 128), F32), tok, tok, tok, tok, tok,
                pltpu.VMEM((n, 3 * d), BF16),
                pltpu.VMEM((d, d), F32), pltpu.VMEM((d, d), BF16), pltpu.VMEM((d, d), BF16),
                pltpu.VMEM((hd + 8, d), F32), pltpu.VMEM((hd + 8, d), F32), pltpu.VMEM((hd + 8, d), F32),
                pltpu.VMEM((hd + 8, d), F32),
                pltpu.VMEM((hd, d), F32), pltpu.VMEM((hd, d), F32), pltpu.VMEM((hd, d), F32), pltpu.VMEM((hd, d), F32),
                pltpu.VMEM((4, d, d), F32), pltpu.VMEM((4, 2, wrows, d), F32), pltpu.VMEM((4, wrows, d), F32),
                pltpu.VMEM((4, wrows, d), F32), pltpu.VMEM((4, 8, d), F32),
                dma((2 * nb + 5,)), dma((4,)), dma((4,)), dma((12,)), dma((12,)), dma((3,)), dma((3,)),
            ],
            compiler_params=pltpu.CompilerParams(collective_id=0, has_side_effects=True,
                                                 vmem_limit_bytes=40 * 1024 * 1024),
        )(*map(in_hbm, (x, dy, gain, bias, w_qkv, w_out, temperature)))
        return pl.pallas_call(
            finish,
            name='finish',
            out_shape=(sds((n, d), BF16), sds((n, d), BF16), sds((wrows, 3 * d), F32), sds((wrows, d), F32),
                       sds((d,), F32), sds((d,), F32), sds((h,), F32)),
            in_specs=[vmem] * 7,
            out_specs=(hbm, hbm, hbm, hbm, vmem, vmem, vmem),
            scratch_shapes=[dma((4,))],
            compiler_params=pltpu.CompilerParams(vmem_limit_bytes=8 * 1024 * 1024),
        )(*outs)

    return jax.shard_map(local_step, mesh=mesh,
                         in_specs=(row_spec, row_spec, full_spec, full_spec, full_spec, full_spec, full_spec),
                         out_specs=(row_spec, row_spec, row_spec, row_spec, part_spec, part_spec, part_spec),
                         check_vma=False)
```

```python
import functools

import jax
import jax.numpy as jnp
from jax import lax
from jax.experimental import pallas as pl
from jax.experimental.pallas import tpu as pltpu
from jax.sharding import PartitionSpec as P

F32, BF16 = jnp.float32, jnp.bfloat16
MESH = pl.DeviceIdType.MESH
BM = 512
CHUNKS = ((2, 0, 128), (2, 128, 384), (3, 0, 384), (0, 0, 384), (1, 0, 384))
scope = jax.named_scope


def dot_nn(a, b):
    return lax.dot_general(a, b, (((1,), (0,)), ((), ())), preferred_element_type=F32)


def dot_nt(a, b):
    return lax.dot_general(a, b, (((1,), (1,)), ((), ())), preferred_element_type=F32)


def dot_tn(a, b):
    return lax.dot_general(a, b, (((0,), (0,)), ((), ())), preferred_element_type=F32)


def kernel(num_heads, num_sp,
           x_hbm, dy_hbm, gain_hbm, bias_hbm, wqkv_hbm, wout_hbm, temp_hbm,
           out_st, gt_st, gwqkv_ref, gwout_ref, ggain_ref, gbias_ref, gtemp_ref,
           gain_ref, bias_ref, temp_ref, x_v, dy_v, wqkv, wout, u_v, ut_v, xhat, rstd, q_v, k_v, v_v, do_v, o_v, dqkv,
           acc, abd, gbd, g_own, g_rx1, g_sum, g_rx2, d_own, d_rx1, d_sum, d_rx2,
           gw, w_rx1, w_sum, w_rx2, gb,
           in_sem, gs, gr, ws, wr, bs, br):
    rows_n, dim = x_v.shape
    hd = dim // num_heads
    nb = rows_n // BM
    wrows = dim // num_sp
    half = dim // 2
    win = 256
    off = dim - win
    nh = num_heads // 2

    me = lax.axis_index('sp')
    partner = me + 1 - 2 * lax.rem(me, 2)
    peer = lax.rem(me + 2, 4)
    diag = lax.rem(partner + 2, 4)

    def blk(i):
        return slice(i * BM, (i + 1) * BM)

    x_copy = [pltpu.make_async_copy(x_hbm.at[blk(i)], x_v.at[blk(i)], in_sem.at[i]) for i in range(nb)]
    dy_copy = pltpu.make_async_copy(dy_hbm, dy_v, in_sem.at[nb])
    wq_copy = pltpu.make_async_copy(wqkv_hbm, wqkv, in_sem.at[nb + 1])
    wo_copy = pltpu.make_async_copy(wout_hbm, wout, in_sem.at[nb + 2])
    small = [pltpu.make_async_copy(a, b, in_sem.at[nb + 3 + n]) for n, (a, b) in enumerate(
        ((gain_hbm, gain_ref), (bias_hbm, bias_ref), (temp_hbm, temp_ref)))]
    x_copy[0].start()
    for c in small:
        c.start()
    wq_copy.start()
    for i in range(1, nb):
        x_copy[i].start()
    wo_copy.start()
    dy_copy.start()

    barrier = pltpu.get_barrier_semaphore()
    for other in (partner, peer, diag):
        pl.semaphore_signal(barrier, inc=1, device_id={'sp': other}, device_id_type=MESH)

    lane = lax.broadcasted_iota(jnp.int32, (hd, dim), 1)
    row = lax.broadcasted_iota(jnp.int32, (hd, dim), 0)
    head_mask = [(lane >= h * hd) & (lane < (h + 1) * hd) for h in range(num_heads)]

    def fold(a):
        lo = jnp.zeros((hd, win), F32)
        hi = jnp.zeros((hd, win), F32)
        for h in range(nh):
            r = slice(h * hd, (h + 1) * hd)
            lo = jnp.where(head_mask[h][:, :win], a[0, r, :], lo)
            hi = jnp.where(head_mask[h + nh][:, off:], a[1, r, :], hi)
        return jnp.concatenate([lo[:, :off], lo[:, off:] + hi[:, :win - off], hi[:, win - off:]], axis=1)

    def expand(ref, compact):
        ref[0, half:, :] = jnp.zeros((win - half, win), BF16)
        ref[1, :half - off, :] = jnp.zeros((half - off, win), BF16)
        for h in range(nh):
            ref[0, h * hd:(h + 1) * hd, :] = jnp.where(head_mask[h], compact, 0.0).astype(BF16)[:, :win]
            g = h + nh
            r = slice(g * hd - off, (g + 1) * hd - off)
            ref[1, r, :] = jnp.where(head_mask[g], compact, 0.0).astype(BF16)[:, off:]

    def per_head(dot, a, w):
        lo = dot(a[:, :win], w[0])
        hi = dot(a[:, off:], w[1])
        return jnp.concatenate([lo[:, :off], lo[:, off:] + hi[:, :win - off], hi[:, win - off:]], axis=1)

    def head_gram(a, b, first):
        at = a.T
        lo = dot_nn(at[:half], b[:, :win])
        hi = dot_nn(at[half:], b[:, off:])
        if first:
            acc[0] = lo
            acc[1] = hi
        else:
            acc[0] += lo
            acc[1] += hi

    def send(src, dst, ssem, rsem, dev):
        return pltpu.make_async_remote_copy(src_ref=src, dst_ref=dst, send_sem=ssem, recv_sem=rsem,
                                            device_id={'sp': dev}, device_id_type=MESH)

    for c in small:
        c.wait()
    gain = gain_ref[...].reshape(1, dim)
    bias = bias_ref[...].reshape(1, dim)
    inv_d = 1.0 / dim

    def layer_norm(i):
        r = blk(i)
        xf = x_v[r, :].astype(F32)
        cen = xf - jnp.sum(xf, axis=-1, keepdims=True) * inv_d
        var = jnp.sum(cen * cen, axis=-1, keepdims=True) * inv_d
        rs = lax.rsqrt(var + 1e-6)
        xh = cen * rs
        xhat[r, :] = xh
        rstd[r, :] = jnp.broadcast_to(rs, (BM, 128))
        u_v[r, :] = (xh * gain + bias).astype(BF16)

    def project_qk(i):
        r = blk(i)
        qk = dot_nn(u_v[r, :], wqkv[:, :2 * dim]).astype(BF16)
        q_v[r, :] = qk[:, :dim]
        k_v[r, :] = qk[:, dim:]

    def sq_sum(ref, i):
        f = ref[blk(i), :].astype(F32)
        return jnp.sum((f * f).reshape(BM // 8, 8, dim), axis=0)

    sq = sk = jnp.zeros((8, dim), F32)
    with scope('p1'):
        x_copy[0].wait()
        layer_norm(0)
        wq_copy.wait()
        for i in range(nb + 1):
            if i + 1 < nb:
                x_copy[i + 1].wait()
                layer_norm(i + 1)
            if i < nb:
                project_qk(i)
            if i > 0:
                head_gram(k_v[blk(i - 1), :], q_v[blk(i - 1), :], i == 1)
                sq = sq + sq_sum(q_v, i - 1)
                sk = sk + sq_sum(k_v, i - 1)
    with scope('fold'):
        g_own[:hd, :] = fold(acc)
        row8 = lax.broadcasted_iota(jnp.int32, (8, dim), 0)
        g_own[hd:hd + 8, :] = jnp.where(row8 == 0, jnp.sum(sq, axis=0, keepdims=True),
                                        jnp.where(row8 == 1, jnp.sum(sk, axis=0, keepdims=True), 0.0))
    pl.semaphore_wait(barrier, 3)
    g1 = send(g_own, g_rx1, gs.at[0], gr.at[0], partner)
    g1.start()

    def p2(i):
        r = blk(i)
        u = u_v[r, :]
        ut_v[:, r] = u.T
        v_v[r, :] = dot_nn(u, wqkv[:, 2 * dim:]).astype(BF16)
        do_v[r, :] = dot_nt(dy_v[r, :], wout[...]).astype(BF16)

    with scope('p2a'):
        wo_copy.wait()
        dy_copy.wait()
        for i in range(nb // 2):
            p2(i)
    with scope('g1w'):
        g1.wait()
    g_sum[...] = g_own[...] + g_rx1[...]
    g2 = send(g_sum, g_rx2, gs.at[1], gr.at[1], peer)
    g2.start()
    with scope('p2b'):
        for i in range(nb // 2, nb):
            p2(i)
        for i in range(nb):
            head_gram(v_v[blk(i), :], do_v[blk(i), :], i == 0)
    d_own[...] = fold(acc)
    d1 = send(d_own, d_rx1, gs.at[2], gr.at[2], partner)
    d1.start()

    with scope('g2w'):
        g2.wait()
    with scope('A'):
        tot = g_sum[...] + g_rx2[...]
        gram = tot[:hd, :]
        sq_row = tot[hd:hd + 1, :]
        sk_row = tot[hd + 1:hd + 2, :]
        sk_full = jnp.zeros((hd, dim), F32)
        for h in range(num_heads):
            col = jnp.sum(jnp.where(lane == row + h * hd, sk_row, 0.0), axis=1, keepdims=True)
            sk_full = jnp.where(head_mask[h], col, sk_full)
        tau = jnp.zeros((1, dim), F32)
        for h in range(num_heads):
            tau = jnp.where(head_mask[h][:1, :], temp_ref[h], tau)
        denom = jnp.sqrt(sq_row) * jnp.sqrt(sk_full)
        cos = gram / denom
        s = tau * cos
        e = jnp.exp(s - jnp.max(s, axis=0, keepdims=True))
        prob = e / jnp.sum(e, axis=0, keepdims=True)
        expand(abd, prob)

    def pair_send(n, part):
        c, lo, hi = CHUNKS[n]
        rows = pl.ds(pl.multiple_of((partner if part else diag) * wrows, 8), wrows)
        return send(gw.at[c, rows, lo:hi], w_rx1.at[c, part, :, lo:hi], ws.at[3 * n + part], wr.at[3 * n + part], partner)

    def cross_send(n):
        c, lo, hi = CHUNKS[n]
        return send(w_sum.at[c, :, lo:hi], w_rx2.at[c, :, lo:hi], ws.at[3 * n + 2], wr.at[3 * n + 2], peer)

    def pair_start(n):
        pair_send(n, 0).start()
        pair_send(n, 1).start()

    def cross_start(n):
        c, lo, hi = CHUNKS[n]
        with scope(f'cs{n}'):
            pair_send(n, 0).wait()
            rows = pl.ds(pl.multiple_of(peer * wrows, 8), wrows)
            w_sum[c, :, lo:hi] = gw[c, rows, lo:hi] + w_rx1[c, 0, :, lo:hi]
            cross_send(n).start()

    with scope('p3'):
        dqkv[:, 2 * dim:] = per_head(dot_nt, do_v[...], abd).astype(BF16)
    with scope('gw2a'):
        gw[2, :, :128] = dot_nn(ut_v[...], dqkv[:, 2 * dim:2 * dim + 128])
    pair_start(0)
    with scope('d1w'):
        d1.wait()
    d_sum[...] = d_own[...] + d_rx1[...]
    d2 = send(d_sum, d_rx2, gs.at[3], gr.at[3], peer)
    d2.start()
    with scope('gw2b'):
        gw[2, :, 128:] = dot_nn(ut_v[...], dqkv[:, 2 * dim + 128:])
    pair_start(1)
    cross_start(0)

    with scope('p4'):
        o_v[...] = per_head(dot_nn, v_v[...], abd).astype(BF16)
    cross_start(1)
    with scope('gw3'):
        gw[3] = dot_tn(o_v[...], dy_v[...])
    pair_start(2)

    with scope('d2w'):
        d2.wait()
    with scope('dA'):
        da = d_sum[...] + d_rx2[...]
        ds = prob * (da - jnp.sum(prob * da, axis=0, keepdims=True))
        dcos = tau * ds
        t_row = jnp.sum(ds * cos, axis=0, keepdims=True)
        lane_t = lax.broadcasted_iota(jnp.int32, (1, num_heads), 1)
        g_temp = jnp.zeros((1, num_heads), F32)
        for h in range(num_heads):
            val = jnp.sum(jnp.where(head_mask[h][:1, :], t_row, 0.0), axis=1, keepdims=True)
            g_temp = jnp.where(lane_t == h, val, g_temp)
        gtemp_ref[...] = g_temp.reshape(num_heads)
        expand(gbd, dcos / denom)
        z = dcos * cos
        dsq2 = -jnp.sum(z, axis=0, keepdims=True) / sq_row
        sk_grad = jnp.zeros((hd, dim), F32)
        for h in range(num_heads):
            col = jnp.sum(jnp.where(head_mask[h], z, 0.0), axis=1, keepdims=True)
            sk_grad = jnp.where(lane == row + h * hd, col, sk_grad)
        dsk2 = -jnp.sum(sk_grad, axis=0, keepdims=True) / sk_row

    with scope('p5'):
        dqkv[:, :dim] = (per_head(dot_nn, k_v[...], gbd) + q_v[...].astype(F32) * dsq2).astype(BF16)
    cross_start(2)
    with scope('gw0'):
        gw[0] = dot_nn(ut_v[...], dqkv[:, :dim])
    pair_start(3)
    with scope('p6'):
        dqkv[:, dim:2 * dim] = (per_head(dot_nt, q_v[...], gbd) + k_v[...].astype(F32) * dsk2).astype(BF16)
    cross_start(3)
    with scope('gw1'):
        gw[1] = dot_nn(ut_v[...], dqkv[:, dim:2 * dim])
    pair_start(4)

    with scope('p7'):
        for i in range(nb):
            r = blk(i)
            out_st[r, :] = (x_v[r, :].astype(F32) + dot_nn(o_v[r, :], wout[...])).astype(BF16)
    cross_start(4)

    def p8(i, carry):
        gg, gbi = carry
        r = pl.ds(pl.multiple_of(i * BM, BM), BM)
        du = dot_nt(dqkv[r, :], wqkv[...])
        xh = xhat[r, :]
        dux = du * xh
        gg = gg + jnp.sum(dux.reshape(BM // 8, 8, dim), axis=0)
        gbi = gbi + jnp.sum(du.reshape(BM // 8, 8, dim), axis=0)
        m1 = jnp.sum(du * gain, axis=-1, keepdims=True) * inv_d
        m2 = jnp.sum(dux * gain, axis=-1, keepdims=True) * inv_d
        dx = (du * gain - m1 - xh * m2) * rstd[r, :1]
        gt_st[r, :] = (dy_v[r, :].astype(F32) + dx).astype(BF16)
        return gg, gbi

    with scope('p8'):
        zero8 = jnp.zeros((8, dim), F32)
        gg, gbi = lax.fori_loop(0, nb, p8, (zero8, zero8))
        gb[me] = jnp.where(row8 == 0, jnp.sum(gg, axis=0, keepdims=True),
                           jnp.where(row8 == 1, jnp.sum(gbi, axis=0, keepdims=True), 0.0))
    gbc = [send(gb.at[me], gb.at[me], bs.at[n], br.at[n], other) for n, other in enumerate((partner, peer, diag))]
    for c in gbc:
        c.start()

    mine = pl.ds(pl.multiple_of(me * wrows, 8), wrows)
    for n, (c, lo, hi) in enumerate(CHUNKS):
        with scope(f'fin{n}'):
            pair_send(n, 1).wait()
            cross_send(n).wait()
        total = gw[c, mine, lo:hi] + w_rx1[c, 1, :, lo:hi] + w_rx2[c, :, lo:hi]
        if c == 3:
            gwout_ref[:, lo:hi] = total
        else:
            gwqkv_ref[:, c * dim + lo:c * dim + hi] = total
    with scope('gbw'):
        for c in gbc:
            c.wait()
    gsum = (gb[0] + gb[1]) + (gb[2] + gb[3])
    ggain_ref[...] = gsum[0:1, :].reshape(dim)
    gbias_ref[...] = gsum[1:2, :].reshape(dim)


def finish(*refs):
    count = (len(refs) - 1) // 2
    sem = refs[-1]
    copies = [pltpu.make_async_copy(refs[n], refs[count + n], sem.at[n]) for n in range(count)]
    for c in copies:
        c.start()
    for c in copies:
        c.wait()


def solution(mesh):
    row_spec = P(('dp', 'sp'), None)
    part_spec = P('dp')
    full_spec = P()
    num_sp = mesh.shape['sp']

    def local_step(x, dy, gain, bias, w_qkv, w_out, temperature):
        n, d = x.shape
        h = temperature.shape[0]
        hd = d // h
        wrows = d // num_sp
        nb = n // BM
        vmem = pl.BlockSpec(memory_space=pltpu.VMEM)
        hbm = pl.BlockSpec(memory_space=pltpu.HBM)
        tok = pltpu.VMEM((n, d), BF16)
        dma = pltpu.SemaphoreType.DMA
        in_hbm = functools.partial(pltpu.with_memory_space_constraint, memory_space=pltpu.HBM)
        shapes = (((n, d), BF16), ((n, d), BF16), ((wrows, 3 * d), F32), ((wrows, d), F32),
                  ((d,), F32), ((d,), F32), ((h,), F32))
        wide = pltpu.VMEM((hd + 8, d), F32)
        slim = pltpu.VMEM((hd, d), F32)
        outs = pl.pallas_call(
            functools.partial(kernel, h, num_sp),
            name='xca',
            out_shape=tuple(pltpu.VMEM(*s) for s in shapes),
            in_specs=[hbm] * 7,
            out_specs=(vmem,) * 7,
            scratch_shapes=[
                pltpu.VMEM((d,), F32), pltpu.VMEM((d,), F32), pltpu.SMEM((h,), F32),
                tok, tok, pltpu.VMEM((d, 3 * d), BF16), pltpu.VMEM((d, d), BF16), tok, pltpu.VMEM((d, n), BF16),
                pltpu.VMEM((n, d), F32), pltpu.VMEM((n, 128), F32), tok, tok, tok, tok, tok,
                pltpu.VMEM((n, 3 * d), BF16),
                pltpu.VMEM((2, d // 2, 256), F32), pltpu.VMEM((2, 256, 256), BF16), pltpu.VMEM((2, 256, 256), BF16),
                wide, wide, wide, wide, slim, slim, slim, slim,
                pltpu.VMEM((4, d, d), F32), pltpu.VMEM((4, 2, wrows, d), F32), pltpu.VMEM((4, wrows, d), F32),
                pltpu.VMEM((4, wrows, d), F32), pltpu.VMEM((4, 8, d), F32),
                dma((nb + 6,)), dma((4,)), dma((4,)),
                dma((3 * len(CHUNKS),)), dma((3 * len(CHUNKS),)), dma((3,)), dma((3,)),
            ],
            compiler_params=pltpu.CompilerParams(collective_id=0, has_side_effects=True,
                                                 vmem_limit_bytes=44 * 1024 * 1024),
        )(*map(in_hbm, (x, dy, gain, bias, w_qkv, w_out, temperature)))
        return pl.pallas_call(
            finish,
            name='finish',
            out_shape=tuple(jax.ShapeDtypeStruct(*s) for s in shapes),
            in_specs=[vmem] * 7,
            out_specs=(hbm,) * 7,
            scratch_shapes=[dma((7,))],
            compiler_params=pltpu.CompilerParams(vmem_limit_bytes=8 * 1024 * 1024),
        )(*outs)

    return jax.shard_map(local_step, mesh=mesh,
                         in_specs=(row_spec, row_spec, full_spec, full_spec, full_spec, full_spec, full_spec),
                         out_specs=(row_spec, row_spec, row_spec, row_spec, part_spec, part_spec, part_spec),
                         check_vma=False)
```
